32 devices in a mesh: orb: 16 (over z, y, core), grid: 2 (over x).
Axes of the slice: x: 2, y: 2, z: 4, core: 2. Of those that a mesh axis runs over, the one named last changes fastest.
Arguments:
- orbitals: bfloat16 [32, 11520], P('orb', 'grid'), may hold values from -1.5 to 1.5
- occupation: bfloat16 [32], P('orb'), may hold values from 0.29882812 to 1
Outputs:
- potentials: float32 [32, 11520], P('orb', 'grid')
- projectors: float32 [32, 11520], P('orb', 'grid')
The draws below stay inside these ranges and needn't reach their ends.
All inputs are finite; a program needn't handle non-finite values.
Results may differ from the reference program's by a relative error of at most 0.0025.
Values may be sent and summed in bfloat16 or wider, within the bound.
A program may use at most 64 MiB of HBM per device.

```python
import math
import jax
import jax.numpy as jnp
from jax import lax

NX = 20
NY = 24
NZ = 24
NORB = 32
NPTS = 11520


def shard_levels(rng, shape, split, smallest, top_value):
    def one(position, shards_of):
        heights = jax.random.uniform(jax.random.fold_in(jax.random.fold_in(rng, 6), position), (shards_of,), jnp.float32, smallest / len(split), top_value / len(split))
        return jnp.repeat(jnp.exp(heights), shape[position] // shards_of).reshape((-1,) + (1,) * (len(shape) - position - 1))

    factor_of = one(*split[0])
    for cut in split[1:]:
        factor_of = factor_of * one(*cut)
    return factor_of


def centred(own_key, extent, scale, bound, shards=(), held_as=jnp.bfloat16):
    array = jax.random.normal(own_key, extent, jnp.float32) * scale
    if len(shards) > 0:
        array = shard_levels(own_key, extent, shards, -0.22, 0.18) * array
    return jnp.clip(array, min=-bound, max=bound).astype(held_as)


def setup_inputs(seed: int = 0) -> dict:
    key_of = jax.random.split(jax.random.key(seed), 3)
    orbitals = centred(key_of[0], (NORB, NPTS), 0.25, 1.5, ((0, 16), (1, 2)))
    occupation = jnp.clip(0.29882812 + 0.7011719 * jax.random.uniform(key_of[1], (NORB,), jnp.float32) ** shard_levels(key_of[1], (NORB,), ((0, 16),), -0.2, 0.2), 0.29882812, 1.0).astype(jnp.bfloat16)
    return dict(orbitals=orbitals, occupation=occupation)


def hartley_table(length):
    index = jnp.arange(length, dtype=jnp.int32)
    product = index[:, None] * index[None, :] % length
    angle = 2.0 * math.pi / length * product.astype(jnp.float32)
    return (jnp.cos(angle) + jnp.sin(angle)).astype(jnp.bfloat16)

def signed_square(length):
    index = jnp.arange(length, dtype=jnp.int32)
    signed = jnp.where(index <= length // 2, index, index - length).astype(jnp.float32)
    return (2.0 * math.pi * signed / length) ** 2

def coulomb_kernel(size_x, size_y, size_z):
    total = signed_square(size_x)[:, None, None] + signed_square(size_y)[None, :, None] + signed_square(size_z)[None, None, :]
    safe = jnp.where(total > 0, total, 1.0)
    return jnp.where(total > 0, 1.0 / safe, 0.0) / (size_x * size_y * size_z)

def solve_pairs(density, table_x, table_y, table_z, kernel):
    fx = table_x.astype(jnp.float32)
    fy = table_y.astype(jnp.float32)
    fz = table_z.astype(jnp.float32)
    section = jnp.einsum('ax,pxyz->payz', fx, density.astype(jnp.float32)).astype(jnp.bfloat16)
    section = jnp.einsum('by,pxyz->pxbz', fy, section.astype(jnp.float32)).astype(jnp.bfloat16)
    spectrum = jnp.einsum('cz,pxyz->pxyc', fz, section.astype(jnp.float32))
    section = (spectrum * kernel).astype(jnp.bfloat16)
    section = jnp.einsum('cz,pxyz->pxyc', fz, section.astype(jnp.float32)).astype(jnp.bfloat16)
    section = jnp.einsum('by,pxyz->pxbz', fy, section.astype(jnp.float32)).astype(jnp.bfloat16)
    return jnp.einsum('ax,pxyz->payz', fx, section.astype(jnp.float32))

def reference(orbitals, occupation):
    table_x = hartley_table(NX)
    table_y = hartley_table(NY)
    table_z = hartley_table(NZ)
    kernel = coulomb_kernel(NX, NY, NZ)
    source = orbitals.astype(jnp.float32)
    weights = occupation.astype(jnp.float32)
    group = math.gcd(NORB, 32)
    blocks = source.reshape(NORB // group, group, NPTS)
    block_weights = weights.reshape(NORB // group, group)

    def potential_of(target):

        def accumulate(running, inputs):
            block, block_weight = inputs
            density = (target[None, :] * block).astype(jnp.bfloat16).reshape(group, NX, NY, NZ)
            potential = solve_pairs(density, table_x, table_y, table_z, kernel).reshape(group, NPTS)
            return (running - jnp.sum(block_weight[:, None] * potential * block, axis=0), None)
        running, unused = lax.scan(accumulate, jnp.zeros((NPTS,), jnp.float32), (blocks, block_weights))
        return running
    potentials = lax.map(potential_of, source)
    gram = lax.dot_general(source, potentials, (((1,), (1,)), ((), ())), precision=lax.Precision.HIGHEST) / NPTS
    factor = jnp.linalg.cholesky(-gram)
    inverse = lax.linalg.triangular_solve(factor, jnp.eye(NORB, dtype=jnp.float32), left_side=True, lower=True)
    projectors = jnp.dot(inverse, potentials, precision=lax.Precision.HIGHEST)
    return (potentials, projectors)
```

```python
import functools
import math

import jax
import jax.numpy as jnp
import numpy as np
from jax import lax
from jax.experimental import pallas as pl
from jax.experimental.pallas import tpu as pltpu
from jax.sharding import PartitionSpec as P

NX = 20
NY = 24
NZ = 24
NPTS = NX * NY * NZ
PLANE = NY * NZ
HALVES = 2
HX = NX // HALVES
TILE = 8
EDGE = HX - TILE
ROWS = 3 * TILE
LANES = 128
PANEL = 8
BATCH = 8
GROUPS = 3
GROUP = PLANE // GROUPS
WIDE = 256
MESH = pl.DeviceIdType.MESH


def hartley_table(length):
    index = np.arange(length, dtype=np.int32)
    product = index[:, None] * index[None, :] % length
    angle = np.float32(2.0 * math.pi / length) * product.astype(np.float32)
    return np.cos(angle) + np.sin(angle)


def signed_square(length):
    index = np.arange(length, dtype=np.int32)
    signed = np.where(index <= length // 2, index, index - length).astype(np.float32)
    return (np.float32(2.0 * math.pi) * signed / np.float32(length)) ** 2


def padded_rows(array):
    zero = np.zeros((TILE - 2 * EDGE,) + array.shape[1:], array.dtype)
    first, second = array[:HX], array[HX:]
    parts = [first[:TILE], first[TILE:], second[TILE:], zero, second[:TILE]]
    return np.concatenate(parts, axis=0)


def grouped(array):
    rows = array.reshape((GROUPS, GROUP) + array.shape[1:])
    wide = np.zeros((GROUPS, WIDE - GROUP) + array.shape[1:], array.dtype)
    return np.concatenate([rows, wide], axis=1).reshape((GROUPS * WIDE,) + array.shape[1:])


def tables():
    eye = np.eye(BATCH, dtype=np.float32)
    table_x = padded_rows(hartley_table(NX))
    table_y = grouped(np.kron(hartley_table(NY), np.eye(NZ, dtype=np.float32)))
    table_z = np.zeros((WIDE, WIDE), np.float32)
    table_z[:GROUP, :GROUP] = np.kron(np.eye(GROUP // NZ), hartley_table(NZ))
    total = (
        signed_square(NX)[:, None, None]
        + signed_square(NY)[None, :, None]
        + signed_square(NZ)[None, None, :]
    )
    safe = np.where(total > 0, total, 1.0)
    kernel = np.where(total > 0, 1.0 / safe, 0.0) / NPTS
    kernel = grouped(kernel.reshape(NX, PLANE).astype(np.float32).T).T
    kernel = kernel.reshape(NX, GROUPS, WIDE).transpose(1, 0, 2)
    kernel = np.tile(kernel, (1, BATCH, 1))
    bf16 = jnp.bfloat16
    return (
        jnp.asarray(np.kron(eye, table_x.T), bf16),
        jnp.asarray(np.kron(eye, table_x), bf16),
        jnp.asarray(table_y.T, bf16),
        jnp.asarray(table_y, bf16),
        jnp.asarray(table_z, bf16),
        jnp.asarray(kernel, jnp.float32),
    )


def column_of(matrix, k):
    if isinstance(k, int):
        return matrix[:, k : k + 1]
    lane = lax.broadcasted_iota(jnp.int32, matrix.shape, 1)
    return jnp.sum(jnp.where(lane == k, matrix, 0.0), axis=1, keepdims=True)


def row_of(matrix, k):
    if isinstance(k, int):
        return matrix[k : k + 1, :]
    line = lax.broadcasted_iota(jnp.int32, matrix.shape, 0)
    return jnp.sum(jnp.where(line == k, matrix, 0.0), axis=0, keepdims=True)


def loop(count, body, carry, most=64):
    if count <= most:
        for k in range(count):
            carry = body(k, carry)
        return carry
    return lax.fori_loop(0, count, body, carry)


def body(
    cols,
    own_hbm,
    occ_hbm,
    xf_hbm,
    xi_hbm,
    yf_hbm,
    yi_hbm,
    tz_hbm,
    k_hbm,
    pot_ref,
    proj_ref,
    own_ref,
    occ_ref,
    s_own,
    xf_ref,
    xi_ref,
    yf_ref,
    yi_ref,
    tz_ref,
    k_ref,
    src,
    part,
    part_in,
    pots,
    pedge,
    edge_out,
    edge_in,
    rowsum,
    gown,
    gall,
    gmat,
    s_tab,
    sent,
    r_x,
    r_col,
    r_y,
    r_core,
    r_p,
    r_g,
    t_col,
    t_yin,
    t_core,
):
    o = lax.axis_index("orb")
    g = lax.axis_index("grid")
    n_orb = 4 * cols
    n = 2 * n_orb
    r = o // 4
    y = (o % 4) // 2
    c = o % 2
    h = 1 - g
    f32 = jnp.float32
    bf16 = jnp.bfloat16
    o_y = r * 4 + (1 - y) * 2 + c
    o_c = r * 4 + y * 2 + (1 - c)

    inputs = [
        pltpu.make_async_copy(a, b, s_own)
        for a, b in ((own_hbm, own_ref), (occ_hbm, occ_ref))
    ]
    for load in inputs:
        load.start()
    loads = [
        pltpu.make_async_copy(a, b, s_tab)
        for a, b in (
            (xf_hbm, xf_ref),
            (yf_hbm, yf_ref),
            (tz_hbm, tz_ref),
            (k_hbm, k_ref),
            (yi_hbm, yi_ref),
            (xi_hbm, xi_ref),
        )
    ]
    barrier = pltpu.get_barrier_semaphore()

    def greet(orb, grid):
        pl.semaphore_signal(barrier, inc=1, device_id=(orb, grid), device_id_type=MESH)

    @pl.loop(1, cols)
    def _(d):
        greet((r + d) % cols * 4 + y * 2 + c, g)

    greet(o, h)
    greet(o_y, g)
    greet(o_c, g)

    for load in loads:
        load.start()
    for load in inputs:
        load.wait()
    own = own_ref[...].astype(f32)
    occ = occ_ref[...].astype(f32)
    own_edges = []
    for t in range(2):
        lines = [own[t : t + 1, PLANE * x : PLANE * (x + 1)] for x in range(HX)]
        src[r, y, c, t, 2 * g] = jnp.concatenate(lines[:TILE], axis=0).astype(bf16)
        own_edges += lines[TILE:]
    own_edges = jnp.concatenate(own_edges + [jnp.zeros((2 * EDGE, PLANE), f32)], axis=0)
    edge_out[...] = own_edges.astype(bf16)

    pl.semaphore_wait(barrier, cols + 2)

    def copy(source, target, send, recv, orb, grid):
        return pltpu.make_async_remote_copy(
            src_ref=source,
            dst_ref=target,
            send_sem=send,
            recv_sem=recv,
            device_id=(orb, grid),
            device_id_type=MESH,
        )

    def piece(j, q, u, w):
        if j == 0:
            return src.at[q, u, w, g, 2 * g]
        if j == 1:
            return src.at[q, u, w, g, pl.ds(h, 2)]
        return src.at[q, u, w, h, pl.ds(g, 2)]

    def same(ref, send, recv, orb):
        return copy(ref, ref, send, recv, orb, g)

    def to_column(j, d):
        q = (r + d) % cols
        return same(piece(j, r, y, c), sent, r_col.at[j, r], q * 4 + y * 2 + c)

    def to_y(j, q):
        return same(piece(j, q, y, c), sent, r_y.at[j, q], o_y)

    def to_core(j, q, u):
        return same(piece(j, q, u, c), sent, r_core.at[j, u], o_c)

    def arrived(j, q, u, w, recv):
        same(piece(j, q, u, w), sent, recv, o_c).wait_recv()

    everyone = pl.ds(0, cols)
    others = pl.ds(0, cols - 1)
    both = pl.ds(0, 2)

    def crossing(half):
        tile = src.at[r, y, c, :, 2 * half]
        return copy(tile, tile, sent, r_x.at[0], o, h)

    crosses = (crossing(g), copy(edge_out, edge_in, sent, r_x.at[1], o, h))
    for cross in crosses:
        cross.start()

    def send_own(j):
        @pl.loop(1, cols)
        def _(d):
            to_column(j, cols - d).start()

        to_y(j, r).start()
        to_core(j, r, y).start()

    send_own(0)
    crossing(h).wait_recv()
    crosses[1].wait_recv()
    second_half = g.astype(f32)
    first_half = 1.0 - second_half
    edges = edge_in[...].astype(f32)
    low = own_edges * first_half + edges * second_half
    high = edges * first_half + own_edges * second_half
    for t in range(2):
        own_lines = slice(EDGE * t, EDGE * (t + 1))
        lines = [low[own_lines], high[own_lines]]
        lines.append(jnp.broadcast_to(occ[:, t : t + 1], (1, PLANE)))
        lines.append(jnp.zeros((TILE - 2 * EDGE - 1, PLANE), f32))
        src[r, y, c, t, 1] = jnp.concatenate(lines, axis=0).astype(bf16)
    send_own(1)

    def relay_column(j):
        @pl.loop(1, cols)
        def _(d):
            q = (r + d) % cols
            arrived(j, q, y, c, r_col.at[j, q])
            to_y(j, q).start()
            to_core(j, q, y).start()

    def relay_y(j):
        @pl.loop(0, cols)
        def _(d):
            q = (r + d) % cols
            arrived(j, q, 1 - y, c, r_y.at[j, q])
            to_core(j, q, 1 - y).start()

    def other_core(j, u):
        arrived(j, everyone, u, 1 - c, r_core.at[j, u])

    relay_column(0)
    relay_column(1)
    send_own(2)
    for load in loads:
        load.wait()
    other_core(0, y)
    other_core(1, y)

    xf = xf_ref[...]
    xi = xi_ref[...]
    yf = yf_ref[...]
    yi = yi_ref[...]
    tz = tz_ref[...]
    kern = k_ref[...]

    def mm(a, b):
        return jnp.dot(a, b, preferred_element_type=f32)

    per = BATCH // 2
    block = (BATCH, ROWS, PLANE)
    flat_block = (BATCH * ROWS, PLANE)
    steps = cols // per
    slabs = BATCH * NX

    def one_batch(u, step, ts, first):
        raw = src[pl.ds(step * per, per), u, :, g].reshape(BATCH * 3, TILE, PLANE)
        raw = raw.astype(f32).reshape(block)
        weight = raw[:, TILE + 2 * EDGE : TILE + 2 * EDGE + 1, :]
        parts = []
        for t in ts:
            target = src[r, y, c, t].astype(f32).reshape(block[1:])
            density = (raw * target[None]).reshape(flat_block).astype(bf16)
            parts.append(mm(xf, density).astype(bf16))
        count = len(ts) * slabs
        s = mm(jnp.concatenate(parts, axis=0), yf).astype(bf16)
        s = [s[:, WIDE * k : WIDE * (k + 1)] for k in range(GROUPS)]
        s = mm(jnp.concatenate(s, axis=0), tz)
        s = s.reshape(GROUPS, len(ts), slabs, WIDE) * jnp.stack([kern] * len(ts), axis=1)
        s = s.reshape(GROUPS * count, WIDE).astype(bf16)
        s = mm(s, tz).astype(bf16)
        s = [s[count * k : count * (k + 1)] for k in range(GROUPS)]
        s = mm(jnp.concatenate(s, axis=1), yi).astype(bf16)
        for k, t in enumerate(ts):
            v = mm(xi, s[slabs * k : slabs * (k + 1)]).reshape(block)
            total = jnp.sum(weight * v * raw, axis=0).reshape(3, TILE, PLANE)
            if first:
                part[t] = -total
            else:
                part[t] -= total

    def batches(u, ts, first):
        if first:
            one_batch(u, 0, ts, True)
        if steps > int(first):

            @pl.loop(int(first), steps)
            def _(k):
                one_batch(u, k, ts, False)

    batches(y, (0, 1), True)
    relay_y(0)
    relay_y(1)
    relay_column(2)
    other_core(0, 1 - y)
    other_core(1, 1 - y)
    batches(1 - y, (0,), False)

    def swap(t):
        return copy(part.at[t, pl.ds(h, 2)], part_in.at[t], sent, r_p.at[t], o, h)

    swap(0).start()
    batches(1 - y, (1,), False)
    swap(1).start()

    relay_y(2)

    def pot_at(t, q, u, w):
        return pedge.at[q, u, w] if t == 2 else pots.at[q, u, w, t]

    def pot_column(t, d):
        q = (r + d) % cols
        return same(pot_at(t, r, y, c), sent, t_col.at[t, r], q * 4 + y * 2 + c)

    def pot_y(t, q):
        return same(pot_at(t, q, y, c), sent, t_yin.at[t, q], o_y)

    def pot_core(t, q, u):
        return same(pot_at(t, q, u, c), sent, t_core.at[t, u], o_c)

    def pot_arrived(t, q, u, w, recv):
        same(pot_at(t, q, u, w), sent, recv, o_c).wait_recv()

    def send_pots(t):
        @pl.loop(1, cols)
        def _(d):
            pot_column(t, cols - d).start()

        pot_y(t, r).start()
        pot_core(t, r, y).start()

    def gram_rows(t, value):
        @pl.loop(0, cols)
        def _(q):
            rows = src[q, :, :, :, 2 * g].reshape(8, TILE, PLANE).astype(f32)
            ends = src[q, :, :, :, 1].reshape(8, TILE, PLANE).astype(f32)
            sums = rows * value[0][None] + ends * value[2][None]
            fold = sums[:, :, :LANES]
            for k in range(LANES, PLANE - LANES + 1, LANES):
                fold += sums[:, :, k : k + LANES]
            tail = PLANE % LANES
            if tail:
                last = jnp.zeros((8, TILE, LANES - tail), f32)
                fold += jnp.concatenate([sums[:, :, PLANE - tail :], last], axis=2)
            fold = jnp.sum(fold, axis=1)
            rowsum[t, pl.ds(pl.multiple_of(q * 8, 8), 8), :] = fold

        gown[t : t + 1, :] = jnp.sum(rowsum[t].T, axis=0, keepdims=True)

    def finish(t):
        swap(t).wait_recv()
        tile = part[t, 2 * g] + part_in[t, g]
        pots[r, y, c, t] = tile.astype(bf16)
        rest = part[t, 1] + part_in[t, h]
        edge = rest[:EDGE] * first_half + rest[EDGE : 2 * EDGE] * second_half
        line = lax.broadcasted_iota(jnp.int32, (TILE, PLANE), 0)
        return tile, edge, jnp.where(line // EDGE == g, rest, 0.0)

    value0 = finish(0)
    send_pots(0)
    other_core(2, y)
    other_core(2, 1 - y)
    gram_rows(0, value0)
    value1 = finish(1)
    send_pots(1)
    gram_rows(1, value1)
    gall[g * n_orb + o] = gown[...]

    def gram_to(dr, dy, dc, dg):
        orb = (r + dr) % cols * 4 + (y + dy) % 2 * 2 + (c + dc) % 2
        row = gall.at[g * n_orb + o]
        return copy(gown, row, sent, r_g, orb, (g + dg) % 2)

    corners = [(a, b, d) for a in (1, 0) for b in (1, 0) for d in (0, 1)]
    if cols <= 4:
        for dr in (cols - 1, *range(1, cols - 1), 0):
            for corner in corners:
                if (dr, *corner) != (0, 0, 0, 0):
                    dy, dg, dc = corner
                    gram_to(dr, dy, dc, dg).start()
    else:
        for dy, dg, dc in corners:
            first = int((dy, dg, dc) == (0, 0, 0))

            @pl.loop(first, cols)
            def _(dr):
                gram_to(dr, dy, dc, dg).start()

    pedge[r, y, c] = jnp.concatenate([value0[1], value1[1]], axis=0).astype(bf16)
    send_pots(2)

    def write(ref, t, value):
        for x in range(0, HX, 2):
            pair = jnp.concatenate([value[x : x + 1], value[x + 1 : x + 2]], axis=1)
            ref[t : t + 1, PLANE * x : PLANE * (x + 2)] = pair

    write(pot_ref, 0, jnp.concatenate(value0[:2], axis=0))
    write(pot_ref, 1, jnp.concatenate(value1[:2], axis=0))

    def pot_relay_column(t):
        @pl.loop(1, cols)
        def _(d):
            q = (r + d) % cols
            pot_arrived(t, q, y, c, t_col.at[t, q])
            pot_y(t, q).start()
            pot_core(t, q, y).start()

    def pot_relay_y(t):
        @pl.loop(0, cols)
        def _(d):
            q = (r + d) % cols
            pot_arrived(t, q, 1 - y, c, t_yin.at[t, q])
            pot_core(t, q, 1 - y).start()

    pot_relay_column(0)
    pot_relay_column(1)
    pot_relay_column(2)
    pot_relay_y(0)

    received = gall.at[pl.ds(0, 2 * n_orb - 1)]
    grams = copy(received, received, sent, r_g, o_c, g)
    grams.wait_recv()

    def assemble(k, carry):
        pairs = [gall[4 * k + j] + gall[n_orb + 4 * k + j] for j in range(4)]
        start = 8 * k if isinstance(k, int) else pl.multiple_of(8 * k, 8)
        gmat[pl.ds(start, 8), :] = jnp.concatenate(pairs, axis=0)
        return carry

    loop(cols, assemble, 0, 16)
    gram = gmat[...]
    sym = (gram + gram.T) * f32(-0.5 / NPTS)
    row_id = lax.broadcasted_iota(jnp.int32, (n, n), 0)
    eye = (row_id == lax.broadcasted_iota(jnp.int32, (n, n), 1)).astype(f32)
    below = lax.broadcasted_iota(jnp.int32, (n, 1), 0)

    def eliminate(k, pair):
        left, right = pair
        row_l = row_of(left, k)
        scale = 1.0 / column_of(row_l, k)
        factor = jnp.where(below > k, column_of(left, k) * scale, 0.0)
        return left - factor * row_l, right - factor * row_of(right, k)

    def eliminate_panel(start, aug):
        names = range(start, start + PANEL)
        columns = [aug[:, k : k + 1] + jnp.zeros_like(aug) for k in names]
        for i, k in enumerate(names):
            scale = 1.0 / columns[i][k : k + 1]
            factor = jnp.where(below > k, columns[i] * scale, 0.0)
            aug = aug - factor * aug[k : k + 1]
            for j in range(i + 1, PANEL):
                columns[j] = columns[j] - factor * columns[j][k : k + 1]
        return aug

    if 2 * n <= LANES:
        aug = jnp.concatenate([sym, eye], axis=1)
        for k in range(0, n, PANEL):
            aug = eliminate_panel(k, aug)
            if k == n // 2:
                pot_relay_y(1)
                pot_relay_y(2)
        left, right = aug[:, :n], aug[:, n:]
    else:
        pot_relay_y(1)
        pot_relay_y(2)
        left, right = loop(n, eliminate, (sym, eye))

    def inverse_row(k):
        diag = column_of(row_of(left, k), k)
        return row_of(right, k) * (1.0 / jnp.sqrt(diag))

    a0, a1 = inverse_row(2 * o), inverse_row(2 * o + 1)

    for u in range(2):
        for t in range(3):
            pot_arrived(t, everyone, u, 1 - c, t_core.at[t, u])

    orbital = lax.broadcasted_iota(jnp.int32, (1, n), 1)
    others0, others1 = [jnp.where(orbital // 2 == o, 0.0, a) for a in (a0, a1)]

    def add(k, sums):
        where = (k // 4, k % 4 // 2, k % 2)
        if not isinstance(k, int):
            where = (k // 4, lax.rem(k, 4) // 2, lax.rem(k, 2))
        edge = pedge[where].astype(f32)
        tiles = [pots[where + (t,)].astype(f32) for t in range(2)]
        ends = [edge[EDGE * t : EDGE * (t + 1)] for t in range(2)]
        new = []
        for a, (tile, end) in zip((others0, others1), sums):
            for t in range(2):
                factor = column_of(a, 2 * k + t)
                tile, end = tile + factor * tiles[t], end + factor * ends[t]
            new.append((tile, end))
        return tuple(new)

    def own_part(a):
        f0, f1 = column_of(a, 2 * o), column_of(a, 2 * o + 1)
        return tuple(f0 * v0 + f1 * v1 for v0, v1 in zip(value0[:2], value1[:2]))

    proj = loop(n_orb, add, (own_part(a0), own_part(a1)))
    for t in range(2):
        write(proj_ref, t, jnp.concatenate(proj[t], axis=0))

    for cross in crosses:
        cross.wait_send()
    for t in range(2):
        swap(t).wait_send()
    for j in range(3):
        same(piece(j, others, y, c), sent, r_col.at[j, r], o_c).wait_send()
        same(piece(j, everyone, y, c), sent, r_col.at[j, r], o_c).wait_send()
        same(piece(j, everyone, both, c), sent, r_col.at[j, r], o_c).wait_send()
    for t in range(3):
        same(pot_at(t, others, y, c), sent, t_col.at[t, r], o_c).wait_send()
        same(pot_at(t, everyone, y, c), sent, t_col.at[t, r], o_c).wait_send()
        same(pot_at(t, everyone, both, c), sent, t_col.at[t, r], o_c).wait_send()
    grams.wait_send()


def store(pot_ref, proj_ref, pot_out, proj_out, sems):
    copies = [
        pltpu.make_async_copy(a, b, sems.at[i])
        for i, (a, b) in enumerate(((pot_ref, pot_out), (proj_ref, proj_out)))
    ]
    for copy in copies:
        copy.start()
    for copy in copies:
        copy.wait()


def on_device(orbitals, occupation):
    n_orb = lax.axis_size("orb")
    cols = n_orb // 4
    n = 2 * n_orb
    consts = tables()
    f32 = jnp.float32
    bf16 = jnp.bfloat16
    dma = pltpu.SemaphoreType.DMA
    vmem = pl.BlockSpec(memory_space=pltpu.VMEM)
    full = jax.ShapeDtypeStruct(orbitals.shape, f32)
    held = pltpu.VMEM(orbitals.shape, f32)
    pot, proj = pl.pallas_call(
        functools.partial(body, cols),
        out_shape=(held, held),
        in_specs=[pl.BlockSpec(memory_space=pl.ANY)] * 8,
        out_specs=(vmem, vmem),
        scratch_shapes=[
            pltpu.VMEM(orbitals.shape, bf16),
            pltpu.VMEM((1, 2), bf16),
            dma,
            *[pltpu.VMEM(a.shape, a.dtype) for a in consts],
            pltpu.VMEM((cols, 2, 2, 2, 3, TILE, PLANE), bf16),
            pltpu.VMEM((2, 3, TILE, PLANE), f32),
            pltpu.VMEM((2, 2, TILE, PLANE), f32),
            pltpu.VMEM((cols, 2, 2, 2, TILE, PLANE), bf16),
            pltpu.VMEM((cols, 2, 2, 2 * EDGE, PLANE), bf16),
            pltpu.VMEM((TILE, PLANE), bf16),
            pltpu.VMEM((TILE, PLANE), bf16),
            pltpu.VMEM((2, n, LANES), f32),
            pltpu.VMEM((2, n), f32),
            pltpu.VMEM((2 * n_orb, 2, n), f32),
            pltpu.VMEM((n, n), f32),
            dma,
            dma,
            dma((2,)),
            dma((3, cols)),
            dma((3, cols)),
            dma((3, 2)),
            dma((2,)),
            dma,
            dma((3, cols)),
            dma((3, cols)),
            dma((3, 2)),
        ],
        compiler_params=pltpu.CompilerParams(
            collective_id=0, has_side_effects=True, vmem_limit_bytes=60 * 1024 * 1024
        ),
        name="exchange",
    )(orbitals, occupation[None], *consts)
    anywhere = pl.BlockSpec(memory_space=pl.ANY)
    return pl.pallas_call(
        store,
        out_shape=(full, full),
        in_specs=[vmem, vmem],
        out_specs=(anywhere, anywhere),
        scratch_shapes=[dma((2,))],
        name="store",
    )(*[pltpu.with_memory_space_constraint(a, pltpu.VMEM) for a in (pot, proj)])


def solution(mesh):
    return jax.shard_map(
        on_device,
        mesh=mesh,
        in_specs=(P("orb", "grid"), P("orb")),
        out_specs=(P("orb", "grid"), P("orb", "grid")),
        check_vma=False,
    )
```
